16 devices in a mesh: dp: 2 (over y, z), tp: 8 (over x, core).
Axes of the slice: x: 4, y: 2, z: 1, core: 2. Of those that a mesh axis runs over, the one named last changes fastest.
The devices are a block of a 4x4x8 slice.
Arguments:
- x: bfloat16 [5632, 3072], P(('dp', 'tp')), parts along dimension 0
- w_gate: bfloat16 [3072, 8192], P(None, 'tp')
- w_up: bfloat16 [3072, 8192], P(None, 'tp')
- w_down: bfloat16 [8192, 3072], P('tp')
Outputs:
- output: bfloat16 [5632, 3072], P(('dp', 'tp')), parts along dimension 0
There are 2 independent parts. The reference program is written for one: setup_inputs(seed, part) draws one part's arguments, and reference() takes and returns one part's arrays. A program takes and returns all parts, laid end to end along the dimension named above; an argument that names none is the same for every part.
All inputs are finite; a program needn't handle non-finite values.
Results may differ from the reference program's by a relative error of at most 0.016.
Values are sent between devices in bfloat16 or wider.
A program may use at most 768 MiB of HBM per device.

```python
import jax
import jax.numpy as jnp

ROWS = 2816
D = 3072
FF = 8192


def setup_inputs(seed: int = 0, part: int = 0) -> dict:
    kx, kg, ku, kd = jax.random.split(jax.random.key(seed), 4)
    drawn = {
        "x": jax.random.normal(jax.random.fold_in(kx, part), (ROWS, D), jnp.float32),
        "w_gate": jax.random.normal(kg, (D, FF), jnp.float32) * D**-0.5,
        "w_up": jax.random.normal(ku, (D, FF), jnp.float32) * D**-0.5,
        "w_down": jax.random.normal(kd, (FF, D), jnp.float32) * FF**-0.5,
    }
    return {k: v.astype(jnp.bfloat16) for k, v in drawn.items()}


def reference(x, w_gate, w_up, w_down):
    gate = jnp.dot(x, w_gate, preferred_element_type=jnp.float32)
    up = jnp.dot(x, w_up, preferred_element_type=jnp.float32)
    hidden = (jax.nn.silu(gate) * up).astype(jnp.bfloat16)
    return jnp.dot(hidden, w_down, preferred_element_type=jnp.float32).astype(jnp.bfloat16)
```

```python
import functools

import jax
import jax.numpy as jnp
from jax import lax
from jax.experimental import pallas as pl
from jax.experimental.pallas import tpu as pltpu
from jax.sharding import PartitionSpec as P

F32, BF16 = jnp.float32, jnp.bfloat16

HIDDEN_TILE = 256
MODEL_TILE = 768


def tile(n, width):
    return pl.ds(pl.multiple_of(n * width, width), width)


def kernel(
    devices, x_hbm, wg_hbm, wu_hbm, wd_hbm, y_hbm,
    wg, wu, wd, xb, sib, first, pure, second, out, work, kept,
    load_sem, ag_send, ag_recv, pass_send, pass_recv,
    sib_send, sib_recv, first_send, first_recv, pure_send, pure_recv, second_send, second_recv, y_sem,
):
    rows = x_hbm.shape[0]
    half = rows // 2
    hidden, model = wd.shape
    hidden_tiles, model_tiles = hidden // HIDDEN_TILE, model // MODEL_TILE
    chips = devices // 2

    me = lax.axis_index("tp")
    chip, core = me // 2, lax.rem(me, 2)
    right = {"tp": lax.rem(chip + 1, chips) * 2 + core}
    left = {"tp": lax.rem(chip + chips - 1, chips) * 2 + core}
    sibling = {"tp": chip * 2 + 1 - core}

    theirs, ours = pl.ds(0, rows), pl.ds(rows, rows)
    lo, hi = pl.ds(rows, half), pl.ds(rows + half, half)

    def remote(src, dst, send, recv, to):
        return pltpu.make_async_remote_copy(
            src_ref=src, dst_ref=dst, send_sem=send, recv_sem=recv, device_id=to, device_id_type=pl.DeviceIdType.MESH
        )

    loads = [
        pltpu.make_async_copy(src, dst, load_sem.at[i])
        for i, (src, dst) in enumerate([(x_hbm, xb.at[0, ours]), (wg_hbm, wg), (wu_hbm, wu), (wd_hbm, wd)])
    ]
    for load in loads:
        load.start()

    barrier = pltpu.get_barrier_semaphore()
    for peer in (left, right, sibling):
        pl.semaphore_signal(barrier, inc=1, device_id=peer, device_id_type=pl.DeviceIdType.MESH)
    pl.semaphore_wait(barrier, 3)
    loads[0].wait()

    gather = [
        remote(xb.at[0, lo], xb.at[1, lo], ag_send.at[0], ag_recv.at[0], right),
        remote(xb.at[0, hi], xb.at[1, hi], ag_send.at[1], ag_recv.at[1], left),
        remote(xb.at[0, hi], xb.at[2, lo], ag_send.at[2], ag_recv.at[2], right),
        remote(xb.at[0, lo], xb.at[2, hi], ag_send.at[3], ag_recv.at[3], left),
        remote(xb.at[1, lo], xb.at[3, lo], ag_send.at[4], ag_recv.at[4], right),
        remote(xb.at[1, hi], xb.at[3, hi], ag_send.at[5], ag_recv.at[5], left),
    ]
    passes = [
        remote(xb.at[q, ours], xb.at[q, theirs], pass_send.at[q], pass_recv.at[q], sibling) for q in range(4)
    ]
    for copy in gather[:4]:
        copy.start()
    passes[0].start()

    def gate_up(q, keep):
        @pl.loop(0, hidden_tiles)
        def _(n):
            cols = tile(n, HIDDEN_TILE)
            gate = jnp.dot(xb[q], wg[:, cols], preferred_element_type=F32)
            up = jnp.dot(xb[q], wu[:, cols], preferred_element_type=F32)
            h = (jax.nn.silu(gate) * up).astype(BF16)
            work[:, cols] = h[:rows]
            kept[keep, :, cols] = h[rows:]

    def to_sibling(q, n):
        cols = tile(n, MODEL_TILE)
        return remote(xb.at[q, theirs, cols], sib.at[q, :, cols], sib_send.at[q, n], sib_recv.at[q, n], sibling)

    def down_theirs(q):
        @pl.loop(0, model_tiles)
        def _(n):
            cols = tile(n, MODEL_TILE)
            term = jnp.dot(work[...], wd[:, cols], preferred_element_type=F32)
            xb[q, theirs, cols] = term.astype(BF16)
            to_sibling(q, n).start()

    def pair_sum(q, keep, n):
        cols = tile(n, MODEL_TILE)
        term = jnp.dot(kept[keep], wd[:, cols], preferred_element_type=F32)
        to_sibling(q, n).wait_recv()
        return term + sib[q, :, cols].astype(F32)

    top, bottom = pl.ds(0, half), pl.ds(half, half)

    def hops(src, q, dst, send, recv, n, lo_to, hi_to, lo_rows, hi_rows):
        cols = tile(n, MODEL_TILE)
        if q is None:
            lo_src, hi_src = src.at[top, cols], src.at[bottom, cols]
        else:
            lo_src, hi_src = src.at[q, lo, cols], src.at[q, hi, cols]
        return (
            remote(lo_src, dst.at[lo_rows, cols], send.at[0, n], recv.at[0, n], lo_to),
            remote(hi_src, dst.at[hi_rows, cols], send.at[1, n], recv.at[1, n], hi_to),
        )

    def pure_hops(n):
        return hops(out, None, pure, pure_send, pure_recv, n, left, right, top, bottom)

    def first_hops(n):
        return hops(xb, 3, first, first_send, first_recv, n, right, left, bottom, top)

    def second_hops(n):
        return hops(xb, 2, second, second_send, second_recv, n, left, right, bottom, top)

    for load in loads[1:]:
        load.wait()
    passes[0].wait_recv()
    gate_up(0, 0)
    down_theirs(0)

    for copy in gather[:2]:
        copy.wait_recv()
    for copy in gather[4:]:
        copy.start()
    passes[1].start()
    passes[1].wait_recv()
    gate_up(1, 2)
    down_theirs(1)

    @pl.loop(0, model_tiles)
    def _(n):
        out[:, tile(n, MODEL_TILE)] = pair_sum(1, 2, n).astype(BF16)
        for copy in pure_hops(n):
            copy.start()

    for copy in gather[2:4]:
        copy.wait_recv()
    passes[2].start()
    passes[2].wait_recv()
    gate_up(2, 1)
    down_theirs(2)

    for copy in gather[4:]:
        copy.wait_recv()
    passes[3].start()
    passes[3].wait_recv()
    gate_up(3, 2)
    down_theirs(3)
    passes[3].wait_send()

    @pl.loop(0, model_tiles)
    def _(n):
        xb[3, ours, tile(n, MODEL_TILE)] = pair_sum(3, 2, n).astype(BF16)
        for copy in first_hops(n):
            copy.start()

    passes[2].wait_send()

    @pl.loop(0, model_tiles)
    def _(n):
        cols = tile(n, MODEL_TILE)
        total = pair_sum(2, 1, n)
        for copy in first_hops(n):
            copy.wait_recv()
        xb[2, ours, cols] = (total + first[:, cols].astype(F32)).astype(BF16)
        for copy in second_hops(n):
            copy.start()

    for copy in gather[:4]:
        copy.wait_send()
    passes[0].wait_send()

    def store(n):
        cols = tile(n, MODEL_TILE)
        return pltpu.make_async_copy(xb.at[0, ours, cols], y_hbm.at[:, cols], y_sem.at[n])

    @pl.loop(0, model_tiles)
    def _(n):
        cols = tile(n, MODEL_TILE)
        total = pair_sum(0, 0, n)
        for copy in pure_hops(n):
            copy.wait_recv()
        total = total + pure[:, cols].astype(F32)
        for copy in second_hops(n):
            copy.wait_recv()
        xb[0, ours, cols] = (total + second[:, cols].astype(F32)).astype(BF16)
        store(n).start()

    for copy in gather[4:]:
        copy.wait_send()
    passes[1].wait_send()

    @pl.loop(0, model_tiles)
    def _(n):
        for q in range(4):
            to_sibling(q, n).wait_send()
        for copy in (*pure_hops(n), *first_hops(n), *second_hops(n)):
            copy.wait_send()
        store(n).wait()


def solution(mesh):
    devices = mesh.shape["tp"]

    def step(x, w_gate, w_up, w_down):
        rows, model = x.shape
        hidden = w_gate.shape[1]
        tiles = model // MODEL_TILE
        dma = pltpu.SemaphoreType.DMA
        return pl.pallas_call(
            functools.partial(kernel, devices),
            out_shape=jax.ShapeDtypeStruct((rows, model), BF16),
            in_specs=[pl.BlockSpec(memory_space=pl.ANY)] * 4,
            out_specs=pl.BlockSpec(memory_space=pl.ANY),
            scratch_shapes=[
                pltpu.VMEM((model, hidden), BF16),
                pltpu.VMEM((model, hidden), BF16),
                pltpu.VMEM((hidden, model), BF16),
                pltpu.VMEM((4, 2 * rows, model), BF16),
                pltpu.VMEM((4, rows, model), BF16),
                pltpu.VMEM((rows, model), BF16),
                pltpu.VMEM((rows, model), BF16),
                pltpu.VMEM((rows, model), BF16),
                pltpu.VMEM((rows, model), BF16),
                pltpu.VMEM((rows, hidden), BF16),
                pltpu.VMEM((3, rows, hidden), BF16),
                dma((4,)),
                dma((6,)), dma((6,)), dma((4,)), dma((4,)),
                dma((4, tiles)), dma((4, tiles)),
                dma((2, tiles)), dma((2, tiles)),
                dma((2, tiles)), dma((2, tiles)),
                dma((2, tiles)), dma((2, tiles)),
                dma((tiles,)),
            ],
            compiler_params=pltpu.CompilerParams(
                collective_id=0, has_side_effects=True, vmem_limit_bytes=67_043_328
            ),
        )(x, w_gate, w_up, w_down)

    return jax.shard_map(
        step,
        mesh=mesh,
        in_specs=(P(("dp", "tp"), None), P(None, "tp"), P(None, "tp"), P("tp", None)),
        out_specs=P(("dp", "tp"), None),
        check_vma=False,
    )
```

```python
import functools

import jax
import jax.numpy as jnp
from jax import lax
from jax.experimental import pallas as pl
from jax.experimental.pallas import tpu as pltpu
from jax.sharding import PartitionSpec as P

F32, BF16 = jnp.float32, jnp.bfloat16

HIDDEN_TILE = 256
MODEL_TILE = 768
LAST = 256


def tile(n, width):
    return pl.ds(pl.multiple_of(n * width, width), width)


def kernel(
    devices, x_hbm, wg_hbm, wu_hbm, wd_hbm, y,
    wg, wu, wd, xb, sib, first, pure, second, total, work, kept,
    load_sem, ag_send, ag_recv, pass_send, pass_recv,
    sib_send, sib_recv, first_send, first_recv, pure_send, pure_recv, second_send, second_recv,
):
    rows = x_hbm.shape[0]
    half = rows // 2
    hidden, model = wd.shape
    hidden_tiles, model_tiles = hidden // HIDDEN_TILE, model // MODEL_TILE
    chips = devices // 2

    me = lax.axis_index("tp")
    chip, core = me // 2, lax.rem(me, 2)
    right = {"tp": lax.rem(chip + 1, chips) * 2 + core}
    left = {"tp": lax.rem(chip + chips - 1, chips) * 2 + core}
    sibling = {"tp": chip * 2 + 1 - core}

    theirs, ours = pl.ds(0, rows), pl.ds(rows, rows)
    lo, hi = pl.ds(rows, half), pl.ds(rows + half, half)

    def remote(src, dst, send, recv, to):
        return pltpu.make_async_remote_copy(
            src_ref=src, dst_ref=dst, send_sem=send, recv_sem=recv, device_id=to, device_id_type=pl.DeviceIdType.MESH
        )

    loads = [
        pltpu.make_async_copy(src, dst, load_sem.at[i])
        for i, (src, dst) in enumerate([(x_hbm, xb.at[0, ours]), (wg_hbm, wg), (wu_hbm, wu), (wd_hbm, wd)])
    ]

    barrier = pltpu.get_barrier_semaphore()
    for peer in (left, right, sibling):
        pl.semaphore_signal(barrier, inc=1, device_id=peer, device_id_type=pl.DeviceIdType.MESH)
    pl.semaphore_wait(barrier, 3)

    top, bottom = pl.ds(0, half), pl.ds(half, half)
    early = [
        remote(x_hbm.at[top], xb.at[1, lo], ag_send.at[0], ag_recv.at[0], right),
        remote(x_hbm.at[bottom], xb.at[1, hi], ag_send.at[1], ag_recv.at[1], left),
    ]
    late = [
        remote(x_hbm.at[bottom], xb.at[2, lo], ag_send.at[2], ag_recv.at[2], right),
        remote(x_hbm.at[top], xb.at[2, hi], ag_send.at[3], ag_recv.at[3], left),
    ]
    relays = [
        remote(xb.at[1, lo], xb.at[3, lo], ag_send.at[4], ag_recv.at[4], right),
        remote(xb.at[1, hi], xb.at[3, hi], ag_send.at[5], ag_recv.at[5], left),
    ]
    passes = [
        remote(xb.at[q, ours] if q else x_hbm, xb.at[q, theirs], pass_send.at[q], pass_recv.at[q], sibling) for q in range(4)
    ]
    for copy in (*early, *late, passes[0], *loads):
        copy.start()

    def gate_up(q, keep):
        @pl.loop(0, hidden_tiles)
        def _(n):
            cols = tile(n, HIDDEN_TILE)
            gate = jnp.dot(xb[q], wg[:, cols], preferred_element_type=F32)
            up = jnp.dot(xb[q], wu[:, cols], preferred_element_type=F32)
            h = (jax.nn.silu(gate) * up).astype(BF16)
            work[:, cols] = h[:rows]
            kept[keep, :, cols] = h[rows:]

    def to_sibling(q, n):
        cols = tile(n, MODEL_TILE)
        return remote(xb.at[q, theirs, cols], sib.at[q, :, cols], sib_send.at[q, n], sib_recv.at[q, n], sibling)

    def down_theirs(q):
        @pl.loop(0, model_tiles)
        def _(n):
            cols = tile(n, MODEL_TILE)
            term = jnp.dot(work[...], wd[:, cols], preferred_element_type=F32)
            xb[q, theirs, cols] = term.astype(BF16)
            to_sibling(q, n).start()

    def from_sibling(q):
        @pl.loop(0, model_tiles)
        def _(n):
            to_sibling(q, n).wait_recv()

    def pair_sum(q, keep, cols):
        term = jnp.dot(kept[keep], wd[:, cols], preferred_element_type=F32)
        return term + sib[q, :, cols].astype(F32)

    def pure_hops():
        return (
            remote(xb.at[0, top], pure.at[top], pure_send.at[0], pure_recv.at[0], left),
            remote(xb.at[0, bottom], pure.at[bottom], pure_send.at[1], pure_recv.at[1], right),
        )

    def first_hops(n):
        cols = pl.ds(n * model // 2, model // 2)
        return (
            remote(xb.at[3, lo, cols], first.at[bottom, cols], first_send.at[0, n], first_recv.at[0, n], right),
            remote(xb.at[3, hi, cols], first.at[top, cols], first_send.at[1, n], first_recv.at[1, n], left),
        )

    ends = [(0, model // 2), (model // 2, model - LAST), (model - LAST, model)]
    pieces = [[pl.ds(c, min(MODEL_TILE, end - c)) for c in range(start, end, MODEL_TILE)] for start, end in ends]

    def second_hops(n):
        cols = pl.ds(ends[n][0], ends[n][1] - ends[n][0])
        return (
            remote(xb.at[2, lo, cols], second.at[bottom, cols], second_send.at[0, n], second_recv.at[0, n], left),
            remote(xb.at[2, hi, cols], second.at[top, cols], second_send.at[1, n], second_recv.at[1, n], right),
        )

    for load in loads:
        load.wait()
    passes[0].wait_recv()
    gate_up(0, 0)
    down_theirs(0)

    for copy in early:
        copy.wait_recv()
    for copy in (*relays, passes[1]):
        copy.start()
    passes[1].wait_recv()
    gate_up(1, 2)
    down_theirs(1)
    from_sibling(1)

    @pl.loop(0, model_tiles)
    def _(n):
        cols = tile(n, MODEL_TILE)
        to_sibling(0, n).wait_send()
        xb[0, theirs, cols] = pair_sum(1, 2, cols).astype(BF16)

    for copy in pure_hops():
        copy.start()

    for copy in late:
        copy.wait_recv()
    passes[2].start()
    passes[2].wait_recv()
    gate_up(2, 1)
    down_theirs(2)

    for copy in relays:
        copy.wait_recv()
    passes[3].start()
    passes[3].wait_recv()
    gate_up(3, 2)
    down_theirs(3)
    passes[3].wait_send()
    from_sibling(3)

    for n in range(2):

        @pl.loop(n * model_tiles // 2, (n + 1) * model_tiles // 2)
        def _(m):
            cols = tile(m, MODEL_TILE)
            xb[3, ours, cols] = pair_sum(3, 2, cols).astype(BF16)

        for copy in first_hops(n):
            copy.start()

    passes[2].wait_send()
    from_sibling(2)
    for n, columns in enumerate(pieces):
        for i, cols in enumerate(columns):
            held = pair_sum(2, 1, cols)
            if n < 2 and i == 0:
                for copy in first_hops(n):
                    copy.wait_recv()
            xb[2, ours, cols] = (held + first[:, cols].astype(F32)).astype(BF16)
        for copy in second_hops(n):
            copy.start()

    from_sibling(0)
    for copy in pure_hops():
        copy.wait_recv()

    @pl.loop(0, model_tiles)
    def _(n):
        cols = tile(n, MODEL_TILE)
        total[:, cols] = pair_sum(0, 0, cols) + pure[:, cols].astype(F32)

    for n, columns in enumerate(pieces):
        for copy in second_hops(n):
            copy.wait_recv()
        for cols in columns:
            y[:, cols] = (total[:, cols] + second[:, cols].astype(F32)).astype(BF16)

    for copy in (*early, *late, *relays, *passes[:2], *pure_hops(), *first_hops(0), *first_hops(1)):
        copy.wait_send()
    for n in range(3):
        for copy in second_hops(n):
            copy.wait_send()

    @pl.loop(0, model_tiles)
    def _(n):
        for q in range(1, 4):
            to_sibling(q, n).wait_send()


def solution(mesh):
    devices = mesh.shape["tp"]

    def step(x, w_gate, w_up, w_down):
        rows, model = x.shape
        hidden = w_gate.shape[1]
        tiles = model // MODEL_TILE
        dma = pltpu.SemaphoreType.DMA
        return pl.pallas_call(
            functools.partial(kernel, devices),
            out_shape=pltpu.VMEM((rows, model), BF16),
            in_specs=[pl.BlockSpec(memory_space=pl.ANY)] * 4,
            out_specs=pl.BlockSpec(memory_space=pltpu.VMEM),
            scratch_shapes=[
                pltpu.VMEM((model, hidden), BF16),
                pltpu.VMEM((model, hidden), BF16),
                pltpu.VMEM((hidden, model), BF16),
                pltpu.VMEM((4, 2 * rows, model), BF16),
                pltpu.VMEM((4, rows, model), BF16),
                pltpu.VMEM((rows, model), BF16),
                pltpu.VMEM((rows, model), BF16),
                pltpu.VMEM((rows, model), BF16),
                pltpu.VMEM((rows, model), F32),
                pltpu.VMEM((rows, hidden), BF16),
                pltpu.VMEM((3, rows, hidden), BF16),
                dma((4,)),
                dma((6,)), dma((6,)), dma((4,)), dma((4,)),
                dma((4, tiles)), dma((4, tiles)),
                dma((2, 2)), dma((2, 2)),
                dma((2,)), dma((2,)),
                dma((2, 3)), dma((2, 3)),
            ],
            compiler_params=pltpu.CompilerParams(
                collective_id=0, has_side_effects=True, vmem_limit_bytes=64_000_000
            ),
        )(x, w_gate, w_up, w_down)

    return jax.shard_map(
        step,
        mesh=mesh,
        in_specs=(P(("dp", "tp"), None), P(None, "tp"), P(None, "tp"), P("tp", None)),
        out_specs=P(("dp", "tp"), None),
        check_vma=False,
    )
```

```python
import functools

import jax
import jax.numpy as jnp
from jax import lax
from jax.experimental import pallas as pl
from jax.experimental.pallas import tpu as pltpu
from jax.sharding import PartitionSpec as P

F32, BF16 = jnp.float32, jnp.bfloat16

HIDDEN_TILE = 256
MODEL_TILE = 768
LAST = 512
HEAD = 48


def tile(n, width):
    return pl.ds(pl.multiple_of(n * width, width), width)


def kernel(
    devices, x_hbm, wg_hbm, wu_hbm, wd_hbm, y,
    wg, wu, wd, xb, sib, first, pure, second, total, work, kept,
    load_sem, ag_send, ag_recv, pass_send, pass_recv,
    sib_send, sib_recv, first_send, first_recv, pure_send, pure_recv, second_send, second_recv,
):
    rows = x_hbm.shape[0]
    half = rows // 2
    hidden, model = wd.shape
    hidden_tiles, model_tiles = hidden // HIDDEN_TILE, model // MODEL_TILE
    chips = devices // 2

    me = lax.axis_index("tp")
    chip, core = me // 2, lax.rem(me, 2)
    right = {"tp": lax.rem(chip + 1, chips) * 2 + core}
    left = {"tp": lax.rem(chip + chips - 1, chips) * 2 + core}
    sibling = {"tp": chip * 2 + 1 - core}

    theirs, ours = pl.ds(0, rows), pl.ds(rows, rows)
    lo, hi = pl.ds(rows, half), pl.ds(rows + half, half)

    def remote(src, dst, send, recv, to):
        return pltpu.make_async_remote_copy(
            src_ref=src, dst_ref=dst, send_sem=send, recv_sem=recv, device_id=to, device_id_type=pl.DeviceIdType.MESH
        )

    loads = [
        pltpu.make_async_copy(src, dst, load_sem.at[i])
        for i, (src, dst) in enumerate([(x_hbm, xb.at[0, ours]), (wg_hbm, wg), (wu_hbm, wu), (wd_hbm, wd)])
    ]

    barrier = pltpu.get_barrier_semaphore()
    for peer in (left, right, sibling):
        pl.semaphore_signal(barrier, inc=1, device_id=peer, device_id_type=pl.DeviceIdType.MESH)
    pl.semaphore_wait(barrier, 3)

    top, bottom = pl.ds(0, half), pl.ds(half, half)
    early = [
        remote(x_hbm.at[top], xb.at[1, lo], ag_send.at[0], ag_recv.at[0], right),
        remote(x_hbm.at[bottom], xb.at[1, hi], ag_send.at[1], ag_recv.at[1], left),
    ]
    late = [
        remote(x_hbm.at[pl.ds(src + start, size)], xb.at[2, pl.ds(dst + start, size)], ag_send.at[i], ag_recv.at[i], to)
        for i, (src, dst, to, start, size) in enumerate(
            [
                (half, rows, right, 0, HEAD),
                (0, rows + half, left, 0, HEAD),
                (half, rows, right, HEAD, half - HEAD),
                (0, rows + half, left, HEAD, half - HEAD),
            ],
            2,
        )
    ]
    relays = [
        remote(xb.at[1, lo], xb.at[3, lo], ag_send.at[6], ag_recv.at[6], right),
        remote(xb.at[1, hi], xb.at[3, hi], ag_send.at[7], ag_recv.at[7], left),
    ]
    passes = [
        remote(xb.at[q, ours] if q else x_hbm, xb.at[q, theirs], pass_send.at[q], pass_recv.at[q], sibling) for q in range(4)
    ]
    for copy in (*early, *late[:2], passes[0], *loads):
        copy.start()

    def gate_up(q, keep):
        @pl.loop(0, hidden_tiles)
        def _(n):
            cols = tile(n, HIDDEN_TILE)
            gate = jnp.dot(xb[q], wg[:, cols], preferred_element_type=F32)
            up = jnp.dot(xb[q], wu[:, cols], preferred_element_type=F32)
            h = (jax.nn.silu(gate) * up).astype(BF16)
            work[:, cols] = h[:rows]
            kept[keep, :, cols] = h[rows:]

    def to_sibling(q, n):
        cols = tile(n, MODEL_TILE)
        return remote(xb.at[q, theirs, cols], sib.at[q, :, cols], sib_send.at[q, n], sib_recv.at[q, n], sibling)

    def down_theirs(q):
        @pl.loop(0, model_tiles)
        def _(n):
            cols = tile(n, MODEL_TILE)
            term = jnp.dot(work[...], wd[:, cols], preferred_element_type=F32)
            xb[q, theirs, cols] = term.astype(BF16)
            to_sibling(q, n).start()

    def from_sibling(q):
        @pl.loop(0, model_tiles)
        def _(n):
            to_sibling(q, n).wait_recv()

    def pair_sum(q, keep, cols):
        term = jnp.dot(kept[keep], wd[:, cols], preferred_element_type=F32)
        return term + sib[q, :, cols].astype(F32)

    def pure_hops():
        return (
            remote(xb.at[0, top], pure.at[top], pure_send.at[0], pure_recv.at[0], left),
            remote(xb.at[0, bottom], pure.at[bottom], pure_send.at[1], pure_recv.at[1], right),
        )

    pieces = [pl.ds(0, model - LAST), pl.ds(model - LAST, LAST)]

    def first_hops(n):
        cols = pieces[n]
        return (
            remote(xb.at[3, lo, cols], first.at[bottom, cols], first_send.at[0, n], first_recv.at[0, n], right),
            remote(xb.at[3, hi, cols], first.at[top, cols], first_send.at[1, n], first_recv.at[1, n], left),
        )

    def second_hops(n):
        cols = pieces[n]
        return (
            remote(xb.at[2, lo, cols], second.at[bottom, cols], second_send.at[0, n], second_recv.at[0, n], left),
            remote(xb.at[2, hi, cols], second.at[top, cols], second_send.at[1, n], second_recv.at[1, n], right),
        )

    for load in loads:
        load.wait()
    passes[0].wait_recv()
    gate_up(0, 0)
    down_theirs(0)

    for copy in early:
        copy.wait_recv()
    for copy in (*relays, *late[2:], passes[1]):
        copy.start()
    passes[1].wait_recv()
    gate_up(1, 2)
    down_theirs(1)
    from_sibling(1)

    @pl.loop(0, model_tiles)
    def _(n):
        cols = tile(n, MODEL_TILE)
        to_sibling(0, n).wait_send()
        xb[0, theirs, cols] = pair_sum(1, 2, cols).astype(BF16)

    for copy in pure_hops():
        copy.start()

    for copy in relays:
        copy.wait_recv()
    passes[3].start()
    passes[3].wait_recv()
    gate_up(3, 2)
    down_theirs(3)
    passes[3].wait_send()
    from_sibling(3)

    @pl.loop(0, model_tiles)
    def _(n):
        cols = tile(n, MODEL_TILE)
        xb[3, ours, cols] = pair_sum(3, 2, cols).astype(BF16)

    for n in range(2):
        for copy in first_hops(n):
            copy.start()

    for copy in late:
        copy.wait_recv()
    passes[2].start()
    passes[2].wait_recv()
    gate_up(2, 1)
    down_theirs(2)
    passes[2].wait_send()
    from_sibling(2)

    @pl.loop(0, model_tiles)
    def _(n):
        cols = tile(n, MODEL_TILE)
        total[:, cols] = pair_sum(2, 1, cols)

    for n in range(2):
        for copy in first_hops(n):
            copy.wait_recv()
        xb[2, ours, pieces[n]] = (total[:, pieces[n]] + first[:, pieces[n]].astype(F32)).astype(BF16)
        for copy in second_hops(n):
            copy.start()

    from_sibling(0)
    for copy in pure_hops():
        copy.wait_recv()

    @pl.loop(0, model_tiles)
    def _(n):
        cols = tile(n, MODEL_TILE)
        total[:, cols] = pair_sum(0, 0, cols) + pure[:, cols].astype(F32)
        for q in range(1, 4):
            to_sibling(q, n).wait_send()

    for copy in (*early, *late, *relays, *passes[:2], *pure_hops(), *first_hops(0), *first_hops(1)):
        copy.wait_send()
    for n in range(2):
        for copy in second_hops(n):
            copy.wait()
        y[:, pieces[n]] = (total[:, pieces[n]] + second[:, pieces[n]].astype(F32)).astype(BF16)


def solution(mesh):
    devices = mesh.shape["tp"]

    def step(x, w_gate, w_up, w_down):
        rows, model = x.shape
        hidden = w_gate.shape[1]
        tiles = model // MODEL_TILE
        dma = pltpu.SemaphoreType.DMA
        return pl.pallas_call(
            functools.partial(kernel, devices),
            out_shape=pltpu.VMEM((rows, model), BF16),
            in_specs=[pl.BlockSpec(memory_space=pl.ANY)] * 4,
            out_specs=pl.BlockSpec(memory_space=pltpu.VMEM),
            scratch_shapes=[
                pltpu.VMEM((model, hidden), BF16),
                pltpu.VMEM((model, hidden), BF16),
                pltpu.VMEM((hidden, model), BF16),
                pltpu.VMEM((4, 2 * rows, model), BF16),
                pltpu.VMEM((4, rows, model), BF16),
                pltpu.VMEM((rows, model), BF16),
                pltpu.VMEM((rows, model), BF16),
                pltpu.VMEM((rows, model), BF16),
                pltpu.VMEM((rows, model), F32),
                pltpu.VMEM((rows, hidden), BF16),
                pltpu.VMEM((3, rows, hidden), BF16),
                dma((4,)),
                dma((8,)), dma((8,)), dma((4,)), dma((4,)),
                dma((4, tiles)), dma((4, tiles)),
                dma((2, 2)), dma((2, 2)),
                dma((2,)), dma((2,)),
                dma((2, 2)), dma((2, 2)),
            ],
            compiler_params=pltpu.CompilerParams(
                collective_id=0, has_side_effects=True, vmem_limit_bytes=64_000_000
            ),
        )(x, w_gate, w_up, w_down)

    return jax.shard_map(
        step,
        mesh=mesh,
        in_specs=(P(("dp", "tp"), None), P(None, "tp"), P(None, "tp"), P("tp", None)),
        out_specs=P(("dp", "tp"), None),
        check_vma=False,
    )
```

```python
import functools

import jax
import jax.numpy as jnp
from jax import lax
from jax.experimental import pallas as pl
from jax.experimental.pallas import tpu as pltpu
from jax.sharding import PartitionSpec as P

F32, BF16 = jnp.float32, jnp.bfloat16

HIDDEN_TILE = 256
MODEL_TILE = 768
LAST = 512
HEAD = 48


def tile(n, width):
    return pl.ds(pl.multiple_of(n * width, width), width)


def kernel(
    devices, x_hbm, wg_hbm, wu_hbm, wd_hbm, y,
    wg, wu, wd, xb, sib, first, pure, second, total, work, kept,
    load_sem, ag_send, ag_recv, pass_send, pass_recv,
    sib_send, sib_recv, first_send, first_recv, pure_send, pure_recv, second_send, second_recv,
):
    rows = x_hbm.shape[0]
    half = rows // 2
    hidden, model = wd.shape
    hidden_tiles, model_tiles = hidden // HIDDEN_TILE, model // MODEL_TILE
    chips = devices // 2

    me = lax.axis_index("tp")
    chip, core = me // 2, lax.rem(me, 2)
    right = {"tp": lax.rem(chip + 1, chips) * 2 + core}
    left = {"tp": lax.rem(chip + chips - 1, chips) * 2 + core}
    sibling = {"tp": chip * 2 + 1 - core}

    theirs, ours = pl.ds(0, rows), pl.ds(rows, rows)
    lo, hi = pl.ds(rows, half), pl.ds(rows + half, half)

    def remote(src, dst, send, recv, to):
        return pltpu.make_async_remote_copy(
            src_ref=src, dst_ref=dst, send_sem=send, recv_sem=recv, device_id=to, device_id_type=pl.DeviceIdType.MESH
        )

    loads = [
        pltpu.make_async_copy(src, dst, load_sem.at[i])
        for i, (src, dst) in enumerate([(x_hbm, xb.at[0, ours]), (wg_hbm, wg), (wu_hbm, wu), (wd_hbm, wd)])
    ]

    barrier = pltpu.get_barrier_semaphore()

    def greet(peer):
        pl.semaphore_signal(barrier, inc=1, device_id=peer, device_id_type=pl.DeviceIdType.MESH)

    for peer in (left, right):
        greet(peer)

    @pl.when(core == 0)
    def _():
        pl.semaphore_wait(barrier, 3)

    @pl.when(core == 1)
    def _():
        pl.semaphore_wait(barrier, 2)


    top, bottom = pl.ds(0, half), pl.ds(half, half)
    early = [
        remote(x_hbm.at[top], xb.at[1, lo], ag_send.at[0], ag_recv.at[0], right),
        remote(x_hbm.at[bottom], xb.at[1, hi], ag_send.at[1], ag_recv.at[1], left),
    ]
    late = [
        remote(x_hbm.at[pl.ds(src + start, size)], xb.at[2, pl.ds(dst + start, size)], ag_send.at[i], ag_recv.at[i], to)
        for i, (src, dst, to, start, size) in enumerate(
            [
                (half, rows, right, 0, HEAD),
                (0, rows + half, left, 0, HEAD),
                (half, rows, right, HEAD, half - HEAD),
                (0, rows + half, left, HEAD, half - HEAD),
            ],
            2,
        )
    ]
    relays = [
        remote(xb.at[1, lo], xb.at[3, lo], ag_send.at[6], ag_recv.at[6], right),
        remote(xb.at[1, hi], xb.at[3, hi], ag_send.at[7], ag_recv.at[7], left),
    ]
    passes = [
        remote(xb.at[q, ours] if q else x_hbm, xb.at[q, theirs], pass_send.at[q], pass_recv.at[q], sibling) for q in range(4)
    ]
    greet(sibling)
    for copy in (*early, *late[:2]):
        copy.start()

    @pl.when(core == 1)
    def _():
        pl.semaphore_wait(barrier, 1)

    for copy in (passes[0], *loads):
        copy.start()

    def gate_up(q, keep):
        @pl.loop(0, hidden_tiles)
        def _(n):
            cols = tile(n, HIDDEN_TILE)
            gate = jnp.dot(xb[q], wg[:, cols], preferred_element_type=F32)
            up = jnp.dot(xb[q], wu[:, cols], preferred_element_type=F32)
            h = (jax.nn.silu(gate) * up).astype(BF16)
            work[:, cols] = h[:rows]
            kept[keep, :, cols] = h[rows:]

    def to_sibling(q, n):
        cols = tile(n, MODEL_TILE)
        return remote(xb.at[q, theirs, cols], sib.at[q, :, cols], sib_send.at[q, n], sib_recv.at[q, n], sibling)

    def down_theirs(q):
        @pl.loop(0, model_tiles)
        def _(n):
            cols = tile(n, MODEL_TILE)
            term = jnp.dot(work[...], wd[:, cols], preferred_element_type=F32)
            xb[q, theirs, cols] = term.astype(BF16)
            to_sibling(q, n).start()

    def from_sibling(q):
        @pl.loop(0, model_tiles)
        def _(n):
            to_sibling(q, n).wait_recv()

    def pair_sum(q, keep, cols):
        term = jnp.dot(kept[keep], wd[:, cols], preferred_element_type=F32)
        return term + sib[q, :, cols].astype(F32)

    def pure_hops():
        return (
            remote(xb.at[0, top], pure.at[top], pure_send.at[0], pure_recv.at[0], left),
            remote(xb.at[0, bottom], pure.at[bottom], pure_send.at[1], pure_recv.at[1], right),
        )

    pieces = [pl.ds(0, model - LAST), pl.ds(model - LAST, LAST)]

    def first_hops(n):
        cols = pieces[n]
        return (
            remote(xb.at[3, lo, cols], first.at[bottom, cols], first_send.at[0, n], first_recv.at[0, n], right),
            remote(xb.at[3, hi, cols], first.at[top, cols], first_send.at[1, n], first_recv.at[1, n], left),
        )

    def second_hops(n):
        cols = pieces[n]
        return (
            remote(xb.at[2, lo, cols], second.at[bottom, cols], second_send.at[0, n], second_recv.at[0, n], left),
            remote(xb.at[2, hi, cols], second.at[top, cols], second_send.at[1, n], second_recv.at[1, n], right),
        )

    for load in loads:
        load.wait()
    passes[0].wait_recv()
    gate_up(0, 0)
    down_theirs(0)

    for copy in early:
        copy.wait_recv()
    for copy in (*relays, *late[2:], passes[1]):
        copy.start()
    passes[1].wait_recv()
    gate_up(1, 2)
    down_theirs(1)
    from_sibling(1)

    @pl.loop(0, model_tiles)
    def _(n):
        cols = tile(n, MODEL_TILE)
        to_sibling(0, n).wait_send()
        xb[0, theirs, cols] = pair_sum(1, 2, cols).astype(BF16)

    for copy in pure_hops():
        copy.start()

    for copy in relays:
        copy.wait_recv()
    passes[3].start()
    passes[3].wait_recv()
    gate_up(3, 2)
    down_theirs(3)
    passes[3].wait_send()
    from_sibling(3)

    @pl.loop(0, model_tiles)
    def _(n):
        cols = tile(n, MODEL_TILE)
        xb[3, ours, cols] = pair_sum(3, 2, cols).astype(BF16)

    for n in range(2):
        for copy in first_hops(n):
            copy.start()

    for copy in late:
        copy.wait_recv()
    passes[2].start()
    passes[2].wait_recv()
    gate_up(2, 1)
    down_theirs(2)
    passes[2].wait_send()
    from_sibling(2)

    @pl.loop(0, model_tiles)
    def _(n):
        cols = tile(n, MODEL_TILE)
        total[:, cols] = pair_sum(2, 1, cols)

    for n in range(2):
        for copy in first_hops(n):
            copy.wait_recv()
        xb[2, ours, pieces[n]] = (total[:, pieces[n]] + first[:, pieces[n]].astype(F32)).astype(BF16)
        for copy in second_hops(n):
            copy.start()

    from_sibling(0)
    for copy in pure_hops():
        copy.wait_recv()

    @pl.loop(0, model_tiles)
    def _(n):
        cols = tile(n, MODEL_TILE)
        total[:, cols] = pair_sum(0, 0, cols) + pure[:, cols].astype(F32)
        for q in range(1, 4):
            to_sibling(q, n).wait_send()

    for copy in (*early, *late, *relays, *passes[:2], *pure_hops(), *first_hops(0), *first_hops(1)):
        copy.wait_send()
    for n in range(2):
        for copy in second_hops(n):
            copy.wait()
        y[:, pieces[n]] = (total[:, pieces[n]] + second[:, pieces[n]].astype(F32)).astype(BF16)


def solution(mesh):
    devices = mesh.shape["tp"]

    def step(x, w_gate, w_up, w_down):
        rows, model = x.shape
        hidden = w_gate.shape[1]
        tiles = model // MODEL_TILE
        dma = pltpu.SemaphoreType.DMA
        return pl.pallas_call(
            functools.partial(kernel, devices),
            out_shape=pltpu.VMEM((rows, model), BF16),
            in_specs=[pl.BlockSpec(memory_space=pl.ANY)] * 4,
            out_specs=pl.BlockSpec(memory_space=pltpu.VMEM),
            scratch_shapes=[
                pltpu.VMEM((model, hidden), BF16),
                pltpu.VMEM((model, hidden), BF16),
                pltpu.VMEM((hidden, model), BF16),
                pltpu.VMEM((4, 2 * rows, model), BF16),
                pltpu.VMEM((4, rows, model), BF16),
                pltpu.VMEM((rows, model), BF16),
                pltpu.VMEM((rows, model), BF16),
                pltpu.VMEM((rows, model), BF16),
                pltpu.VMEM((rows, model), F32),
                pltpu.VMEM((rows, hidden), BF16),
                pltpu.VMEM((3, rows, hidden), BF16),
                dma((4,)),
                dma((8,)), dma((8,)), dma((4,)), dma((4,)),
                dma((4, tiles)), dma((4, tiles)),
                dma((2, 2)), dma((2, 2)),
                dma((2,)), dma((2,)),
                dma((2, 2)), dma((2, 2)),
            ],
            compiler_params=pltpu.CompilerParams(
                collective_id=0, has_side_effects=True, vmem_limit_bytes=64_000_000
            ),
        )(x, w_gate, w_up, w_down)

    return jax.shard_map(
        step,
        mesh=mesh,
        in_specs=(P(("dp", "tp"), None), P(None, "tp"), P(None, "tp"), P("tp", None)),
        out_specs=P(("dp", "tp"), None),
        check_vma=False,
    )
```

```python
import functools

import jax
import jax.numpy as jnp
from jax import lax
from jax.experimental import pallas as pl
from jax.experimental.pallas import tpu as pltpu
from jax.sharding import PartitionSpec as P

F32, BF16 = jnp.float32, jnp.bfloat16

HIDDEN_TILE = 256
MODEL_TILE = 768
LAST = 512
HEAD = 48


def tile(n, width):
    return pl.ds(pl.multiple_of(n * width, width), width)


def kernel(
    devices, x_hbm, wg_hbm, wu_hbm, wd_hbm, y,
    wg, wu, wd, xb, sib, first, pure, second, total, work, kept,
    load_sem, ag_send, ag_recv, pass_send, pass_recv,
    sib_send, sib_recv, first_send, first_recv, pure_send, pure_recv, second_send, second_recv, seen, mate,
):
    rows = x_hbm.shape[0]
    half = rows // 2
    hidden, model = wd.shape
    hidden_tiles, model_tiles = hidden // HIDDEN_TILE, model // MODEL_TILE
    chips = devices // 2

    me = lax.axis_index("tp")
    chip, core = me // 2, lax.rem(me, 2)
    right = {"tp": lax.rem(chip + 1, chips) * 2 + core}
    left = {"tp": lax.rem(chip + chips - 1, chips) * 2 + core}
    sibling = {"tp": chip * 2 + 1 - core}

    theirs, ours = pl.ds(0, rows), pl.ds(rows, rows)
    lo, hi = pl.ds(rows, half), pl.ds(rows + half, half)

    def remote(src, dst, send, recv, to):
        return pltpu.make_async_remote_copy(
            src_ref=src, dst_ref=dst, send_sem=send, recv_sem=recv, device_id=to, device_id_type=pl.DeviceIdType.MESH
        )

    loads = [
        pltpu.make_async_copy(src, dst, load_sem.at[i])
        for i, (src, dst) in enumerate([(x_hbm, xb.at[0, ours]), (wg_hbm, wg), (wu_hbm, wu), (wd_hbm, wd)])
    ]

    barrier = pltpu.get_barrier_semaphore()

    def greet(peer):
        pl.semaphore_signal(barrier, inc=1, device_id=peer, device_id_type=pl.DeviceIdType.MESH)

    @pl.when(core == 0)
    def _():
        greet(right)
        pl.semaphore_wait(barrier, 2)

    @pl.when(core == 1)
    def _():
        greet(left)
        greet(sibling)
        pl.semaphore_wait(barrier, 1)

    top, bottom = pl.ds(0, half), pl.ds(half, half)
    early = [
        remote(x_hbm.at[top], xb.at[1, lo], ag_send.at[0], ag_recv.at[0], right),
        remote(x_hbm.at[bottom], xb.at[1, hi], ag_send.at[1], ag_recv.at[1], left),
    ]
    late = [
        remote(x_hbm.at[pl.ds(src + start, size)], xb.at[2, pl.ds(dst + start, size)], ag_send.at[i], ag_recv.at[i], to)
        for i, (src, dst, to, start, size) in enumerate(
            [
                (half, rows, right, 0, HEAD),
                (0, rows + half, left, 0, HEAD),
                (half, rows, right, HEAD, half - HEAD),
                (0, rows + half, left, HEAD, half - HEAD),
            ],
            2,
        )
    ]
    relays = [
        remote(xb.at[1, lo], xb.at[3, lo], ag_send.at[6], ag_recv.at[6], right),
        remote(xb.at[1, hi], xb.at[3, hi], ag_send.at[7], ag_recv.at[7], left),
    ]
    passes = [
        remote(xb.at[q, ours] if q else x_hbm, xb.at[q, theirs], pass_send.at[q], pass_recv.at[q], sibling) for q in range(4)
    ]

    def tell(sem, peer):
        pl.semaphore_signal(sem, inc=1, device_id=peer, device_id_type=pl.DeviceIdType.MESH)

    @pl.when(core == 0)
    def _():
        tell(seen, left)
        early[1].start()
        late[1].start()
        tell(mate, sibling)
        passes[0].start()
        pl.semaphore_wait(seen, 1)
        early[0].start()
        late[0].start()

    @pl.when(core == 1)
    def _():
        tell(seen, right)
        early[0].start()
        late[0].start()
        pl.semaphore_wait(seen, 1)
        early[1].start()
        late[1].start()
        pl.semaphore_wait(mate, 1)
        passes[0].start()

    for load in loads:
        load.start()

    def gate_up(q, keep):
        @pl.loop(0, hidden_tiles)
        def _(n):
            cols = tile(n, HIDDEN_TILE)
            gate = jnp.dot(xb[q], wg[:, cols], preferred_element_type=F32)
            up = jnp.dot(xb[q], wu[:, cols], preferred_element_type=F32)
            h = (jax.nn.silu(gate) * up).astype(BF16)
            work[:, cols] = h[:rows]
            kept[keep, :, cols] = h[rows:]

    def to_sibling(q, n):
        cols = tile(n, MODEL_TILE)
        return remote(xb.at[q, theirs, cols], sib.at[q, :, cols], sib_send.at[q, n], sib_recv.at[q, n], sibling)

    def down_theirs(q):
        @pl.loop(0, model_tiles)
        def _(n):
            cols = tile(n, MODEL_TILE)
            term = jnp.dot(work[...], wd[:, cols], preferred_element_type=F32)
            xb[q, theirs, cols] = term.astype(BF16)
            to_sibling(q, n).start()

    def from_sibling(q):
        @pl.loop(0, model_tiles)
        def _(n):
            to_sibling(q, n).wait_recv()

    def pair_sum(q, keep, cols):
        term = jnp.dot(kept[keep], wd[:, cols], preferred_element_type=F32)
        return term + sib[q, :, cols].astype(F32)

    def pure_hops():
        return (
            remote(xb.at[0, top], pure.at[top], pure_send.at[0], pure_recv.at[0], left),
            remote(xb.at[0, bottom], pure.at[bottom], pure_send.at[1], pure_recv.at[1], right),
        )

    pieces = [pl.ds(0, model - LAST), pl.ds(model - LAST, LAST)]

    def first_hops(n):
        cols = pieces[n]
        return (
            remote(xb.at[3, lo, cols], first.at[bottom, cols], first_send.at[0, n], first_recv.at[0, n], right),
            remote(xb.at[3, hi, cols], first.at[top, cols], first_send.at[1, n], first_recv.at[1, n], left),
        )

    def second_hops(n):
        cols = pieces[n]
        return (
            remote(xb.at[2, lo, cols], second.at[bottom, cols], second_send.at[0, n], second_recv.at[0, n], left),
            remote(xb.at[2, hi, cols], second.at[top, cols], second_send.at[1, n], second_recv.at[1, n], right),
        )

    for load in loads:
        load.wait()
    passes[0].wait_recv()
    gate_up(0, 0)
    down_theirs(0)

    for copy in early:
        copy.wait_recv()
    for copy in (*relays, *late[2:], passes[1]):
        copy.start()
    passes[1].wait_recv()
    gate_up(1, 2)
    down_theirs(1)
    from_sibling(1)

    @pl.loop(0, model_tiles)
    def _(n):
        cols = tile(n, MODEL_TILE)
        to_sibling(0, n).wait_send()
        xb[0, theirs, cols] = pair_sum(1, 2, cols).astype(BF16)

    for copy in pure_hops():
        copy.start()

    for copy in relays:
        copy.wait_recv()
    passes[3].start()
    passes[3].wait_recv()
    gate_up(3, 2)
    down_theirs(3)
    passes[3].wait_send()
    from_sibling(3)

    @pl.loop(0, model_tiles)
    def _(n):
        cols = tile(n, MODEL_TILE)
        xb[3, ours, cols] = pair_sum(3, 2, cols).astype(BF16)

    for n in range(2):
        for copy in first_hops(n):
            copy.start()

    for copy in late:
        copy.wait_recv()
    passes[2].start()
    passes[2].wait_recv()
    gate_up(2, 1)
    down_theirs(2)
    passes[2].wait_send()
    from_sibling(2)

    @pl.loop(0, model_tiles)
    def _(n):
        cols = tile(n, MODEL_TILE)
        total[:, cols] = pair_sum(2, 1, cols)

    for n in range(2):
        for copy in first_hops(n):
            copy.wait_recv()
        xb[2, ours, pieces[n]] = (total[:, pieces[n]] + first[:, pieces[n]].astype(F32)).astype(BF16)
        for copy in second_hops(n):
            copy.start()

    from_sibling(0)
    for copy in pure_hops():
        copy.wait_recv()

    @pl.loop(0, model_tiles)
    def _(n):
        cols = tile(n, MODEL_TILE)
        total[:, cols] = pair_sum(0, 0, cols) + pure[:, cols].astype(F32)
        for q in range(1, 4):
            to_sibling(q, n).wait_send()

    for copy in (*early, *late, *relays, *passes[:2], *pure_hops(), *first_hops(0), *first_hops(1)):
        copy.wait_send()
    for n in range(2):
        for copy in second_hops(n):
            copy.wait()
        y[:, pieces[n]] = (total[:, pieces[n]] + second[:, pieces[n]].astype(F32)).astype(BF16)


def solution(mesh):
    devices = mesh.shape["tp"]

    def step(x, w_gate, w_up, w_down):
        rows, model = x.shape
        hidden = w_gate.shape[1]
        tiles = model // MODEL_TILE
        dma = pltpu.SemaphoreType.DMA
        return pl.pallas_call(
            functools.partial(kernel, devices),
            out_shape=pltpu.VMEM((rows, model), BF16),
            in_specs=[pl.BlockSpec(memory_space=pl.ANY)] * 4,
            out_specs=pl.BlockSpec(memory_space=pltpu.VMEM),
            scratch_shapes=[
                pltpu.VMEM((model, hidden), BF16),
                pltpu.VMEM((model, hidden), BF16),
                pltpu.VMEM((hidden, model), BF16),
                pltpu.VMEM((4, 2 * rows, model), BF16),
                pltpu.VMEM((4, rows, model), BF16),
                pltpu.VMEM((rows, model), BF16),
                pltpu.VMEM((rows, model), BF16),
                pltpu.VMEM((rows, model), BF16),
                pltpu.VMEM((rows, model), F32),
                pltpu.VMEM((rows, hidden), BF16),
                pltpu.VMEM((3, rows, hidden), BF16),
                dma((4,)),
                dma((8,)), dma((8,)), dma((4,)), dma((4,)),
                dma((4, tiles)), dma((4, tiles)),
                dma((2, 2)), dma((2, 2)),
                dma((2,)), dma((2,)),
                dma((2, 2)), dma((2, 2)),
                pltpu.SemaphoreType.REGULAR, pltpu.SemaphoreType.REGULAR,
            ],
            compiler_params=pltpu.CompilerParams(
                collective_id=0, has_side_effects=True, vmem_limit_bytes=64_000_000
            ),
        )(x, w_gate, w_up, w_down)

    return jax.shard_map(
        step,
        mesh=mesh,
        in_specs=(P(("dp", "tp"), None), P(None, "tp"), P(None, "tp"), P("tp", None)),
        out_specs=P(("dp", "tp"), None),
        check_vma=False,
    )
```

```python
import functools

import jax
import jax.numpy as jnp
from jax import lax
from jax.experimental import pallas as pl
from jax.experimental.pallas import tpu as pltpu
from jax.sharding import PartitionSpec as P

F32, BF16 = jnp.float32, jnp.bfloat16

HIDDEN_TILE = 256
MODEL_TILE = 768
LAST = 512
HEAD = 48


def tile(n, width):
    return pl.ds(pl.multiple_of(n * width, width), width)


def kernel(
    devices, x_hbm, wg_hbm, wu_hbm, wd_hbm, y,
    wg, wu, wd, xb, sib, first, pure, second, total, work, kept,
    load_sem, ag_send, ag_recv, pass_send, pass_recv,
    sib_send, sib_recv, first_send, first_recv, pure_send, pure_recv, second_send, second_recv, seen, mate,
):
    rows = x_hbm.shape[0]
    half = rows // 2
    hidden, model = wd.shape
    hidden_tiles, model_tiles = hidden // HIDDEN_TILE, model // MODEL_TILE
    chips = devices // 2

    me = lax.axis_index("tp")
    chip, core = me // 2, lax.rem(me, 2)
    right = {"tp": lax.rem(chip + 1, chips) * 2 + core}
    left = {"tp": lax.rem(chip + chips - 1, chips) * 2 + core}
    sibling = {"tp": chip * 2 + 1 - core}

    theirs, ours = pl.ds(0, rows), pl.ds(rows, rows)
    lo, hi = pl.ds(rows, half), pl.ds(rows + half, half)

    def remote(src, dst, send, recv, to):
        return pltpu.make_async_remote_copy(
            src_ref=src, dst_ref=dst, send_sem=send, recv_sem=recv, device_id=to, device_id_type=pl.DeviceIdType.MESH
        )

    loads = [
        pltpu.make_async_copy(src, dst, load_sem.at[i])
        for i, (src, dst) in enumerate([(x_hbm, xb.at[0, ours]), (wg_hbm, wg), (wu_hbm, wu), (wd_hbm, wd)])
    ]

    barrier = pltpu.get_barrier_semaphore()

    def greet(peer):
        pl.semaphore_signal(barrier, inc=1, device_id=peer, device_id_type=pl.DeviceIdType.MESH)

    @pl.when(core == 0)
    def _():
        greet(right)
        pl.semaphore_wait(barrier, 2)

    @pl.when(core == 1)
    def _():
        greet(left)
        greet(sibling)
        pl.semaphore_wait(barrier, 1)

    top, bottom = pl.ds(0, half), pl.ds(half, half)
    early = [
        remote(x_hbm.at[top], xb.at[1, lo], ag_send.at[0], ag_recv.at[0], right),
        remote(x_hbm.at[bottom], xb.at[1, hi], ag_send.at[1], ag_recv.at[1], left),
    ]
    late = [
        remote(x_hbm.at[pl.ds(src + start, size)], xb.at[2, pl.ds(dst + start, size)], ag_send.at[i], ag_recv.at[i], to)
        for i, (src, dst, to, start, size) in enumerate(
            [
                (half, rows, right, 0, HEAD),
                (0, rows + half, left, 0, HEAD),
                (half, rows, right, HEAD, half - HEAD),
                (0, rows + half, left, HEAD, half - HEAD),
            ],
            2,
        )
    ]
    relays = [
        remote(xb.at[1, lo], xb.at[3, lo], ag_send.at[6], ag_recv.at[6], right),
        remote(xb.at[1, hi], xb.at[3, hi], ag_send.at[7], ag_recv.at[7], left),
    ]
    passes = [
        remote(xb.at[q, ours] if q else x_hbm, xb.at[q, theirs], pass_send.at[q], pass_recv.at[q], sibling) for q in range(4)
    ]

    def tell(sem, peer):
        pl.semaphore_signal(sem, inc=1, device_id=peer, device_id_type=pl.DeviceIdType.MESH)

    @pl.when(core == 0)
    def _():
        tell(seen, left)
        early[1].start()
        late[1].start()
        tell(mate, sibling)
        passes[0].start()
        pl.semaphore_wait(seen, 1)
        early[0].start()
        late[0].start()

    @pl.when(core == 1)
    def _():
        tell(seen, right)
        early[0].start()
        late[0].start()
        pl.semaphore_wait(seen, 1)
        early[1].start()
        late[1].start()
        pl.semaphore_wait(mate, 1)
        passes[0].start()

    for load in loads:
        load.start()

    def gate_up(q, keep):
        @pl.loop(0, hidden_tiles)
        def _(n):
            cols = tile(n, HIDDEN_TILE)
            gate = jnp.dot(xb[q], wg[:, cols], preferred_element_type=F32)
            up = jnp.dot(xb[q], wu[:, cols], preferred_element_type=F32)
            h = (jax.nn.silu(gate) * up).astype(BF16)
            work[:, cols] = h[:rows]
            kept[keep, :, cols] = h[rows:]

    def to_sibling(q, n):
        cols = tile(n, MODEL_TILE)
        return remote(xb.at[q, theirs, cols], sib.at[q, :, cols], sib_send.at[q, n], sib_recv.at[q, n], sibling)

    def down_theirs(q):
        @pl.loop(0, model_tiles)
        def _(n):
            cols = tile(n, MODEL_TILE)
            term = jnp.dot(work[...], wd[:, cols], preferred_element_type=F32)
            xb[q, theirs, cols] = term.astype(BF16)
            to_sibling(q, n).start()

    def from_sibling(q):
        @pl.loop(0, model_tiles)
        def _(n):
            to_sibling(q, n).wait_recv()

    def pair_sum(q, keep, cols):
        term = jnp.dot(kept[keep], wd[:, cols], preferred_element_type=F32)
        return term + sib[q, :, cols].astype(F32)

    def pure_hops():
        return (
            remote(xb.at[0, top], pure.at[top], pure_send.at[0], pure_recv.at[0], left),
            remote(xb.at[0, bottom], pure.at[bottom], pure_send.at[1], pure_recv.at[1], right),
        )

    pieces = [pl.ds(0, model - LAST), pl.ds(model - LAST, LAST)]

    def first_hops(n):
        cols = pieces[n]
        return (
            remote(xb.at[3, lo, cols], first.at[bottom, cols], first_send.at[0, n], first_recv.at[0, n], right),
            remote(xb.at[3, hi, cols], first.at[top, cols], first_send.at[1, n], first_recv.at[1, n], left),
        )

    def second_hops(n):
        cols = pieces[n]
        return (
            remote(xb.at[2, lo, cols], second.at[bottom, cols], second_send.at[0, n], second_recv.at[0, n], left),
            remote(xb.at[2, hi, cols], second.at[top, cols], second_send.at[1, n], second_recv.at[1, n], right),
        )

    for load in loads:
        load.wait()
    passes[0].wait_recv()
    gate_up(0, 0)
    down_theirs(0)

    for copy in early:
        copy.wait_recv()
    for copy in (*relays, *late[2:], passes[1]):
        copy.start()
    passes[1].wait_recv()
    gate_up(1, 2)
    down_theirs(1)
    from_sibling(1)

    @pl.loop(0, model_tiles)
    def _(n):
        cols = tile(n, MODEL_TILE)
        to_sibling(0, n).wait_send()
        xb[0, theirs, cols] = pair_sum(1, 2, cols).astype(BF16)

    for copy in pure_hops():
        copy.start()

    for copy in relays:
        copy.wait_recv()
    passes[3].start()
    passes[3].wait_recv()
    gate_up(3, 2)
    down_theirs(3)
    passes[3].wait_send()
    from_sibling(3)

    @pl.loop(0, model_tiles)
    def _(n):
        cols = tile(n, MODEL_TILE)
        xb[3, ours, cols] = pair_sum(3, 2, cols).astype(BF16)

    for n in range(2):
        for copy in first_hops(n):
            copy.start()

    for copy in late:
        copy.wait_recv()
    passes[2].start()
    passes[2].wait_recv()
    gate_up(2, 1)
    down_theirs(2)
    passes[2].wait_send()
    from_sibling(2)

    @pl.loop(0, model_tiles)
    def _(n):
        cols = tile(n, MODEL_TILE)
        total[:, cols] = pair_sum(2, 1, cols)

    for n in range(2):
        for copy in first_hops(n):
            copy.wait_recv()
        xb[2, ours, pieces[n]] = (total[:, pieces[n]] + first[:, pieces[n]].astype(F32)).astype(BF16)
        for copy in second_hops(n):
            copy.start()

    from_sibling(0)
    for copy in pure_hops():
        copy.wait_recv()

    @pl.loop(0, model_tiles)
    def _(n):
        cols = tile(n, MODEL_TILE)
        total[:, cols] = pair_sum(0, 0, cols) + pure[:, cols].astype(F32)
        for q in range(1, 4):
            to_sibling(q, n).wait_send()

    for copy in (*early, *late, *relays, *passes[:2], *pure_hops(), *first_hops(0), *first_hops(1)):
        copy.wait_send()
    for n in range(2):
        for copy, half_rows in zip(second_hops(n), (bottom, top)):
            copy.wait_recv()
            held = total[half_rows, pieces[n]] + second[half_rows, pieces[n]].astype(F32)
            y[half_rows, pieces[n]] = held.astype(BF16)

    for copy in (*second_hops(0), *second_hops(1)):
        copy.wait_send()


def solution(mesh):
    devices = mesh.shape["tp"]

    def step(x, w_gate, w_up, w_down):
        rows, model = x.shape
        hidden = w_gate.shape[1]
        tiles = model // MODEL_TILE
        dma = pltpu.SemaphoreType.DMA
        return pl.pallas_call(
            functools.partial(kernel, devices),
            out_shape=pltpu.VMEM((rows, model), BF16),
            in_specs=[pl.BlockSpec(memory_space=pl.ANY)] * 4,
            out_specs=pl.BlockSpec(memory_space=pltpu.VMEM),
            scratch_shapes=[
                pltpu.VMEM((model, hidden), BF16),
                pltpu.VMEM((model, hidden), BF16),
                pltpu.VMEM((hidden, model), BF16),
                pltpu.VMEM((4, 2 * rows, model), BF16),
                pltpu.VMEM((4, rows, model), BF16),
                pltpu.VMEM((rows, model), BF16),
                pltpu.VMEM((rows, model), BF16),
                pltpu.VMEM((rows, model), BF16),
                pltpu.VMEM((rows, model), F32),
                pltpu.VMEM((rows, hidden), BF16),
                pltpu.VMEM((3, rows, hidden), BF16),
                dma((4,)),
                dma((8,)), dma((8,)), dma((4,)), dma((4,)),
                dma((4, tiles)), dma((4, tiles)),
                dma((2, 2)), dma((2, 2)),
                dma((2,)), dma((2,)),
                dma((2, 2)), dma((2, 2)),
                pltpu.SemaphoreType.REGULAR, pltpu.SemaphoreType.REGULAR,
            ],
            compiler_params=pltpu.CompilerParams(
                collective_id=0, has_side_effects=True, vmem_limit_bytes=64_000_000
            ),
        )(x, w_gate, w_up, w_down)

    return jax.shard_map(
        step,
        mesh=mesh,
        in_specs=(P(("dp", "tp"), None), P(None, "tp"), P(None, "tp"), P("tp", None)),
        out_specs=P(("dp", "tp"), None),
        check_vma=False,
    )
```

```python
import functools

import jax
import jax.numpy as jnp
from jax import lax
from jax.experimental import pallas as pl
from jax.experimental.pallas import tpu as pltpu
from jax.sharding import PartitionSpec as P

F32, BF16 = jnp.float32, jnp.bfloat16

HIDDEN_TILE = 256
MODEL_TILE = 768
LAST = 512
HEAD = 48


def tile(n, width):
    return pl.ds(pl.multiple_of(n * width, width), width)


def kernel(
    devices, x_hbm, wg_hbm, wu_hbm, wd_hbm, y,
    wg, wu, wd, xb, sib, first, pure, second, total, work, kept,
    load_sem, ag_send, ag_recv, pass_send, pass_recv,
    sib_send, sib_recv, first_send, first_recv, pure_send, pure_recv, second_send, second_recv, seen, mate,
):
    rows = x_hbm.shape[0]
    half = rows // 2
    hidden, model = wd.shape
    hidden_tiles, model_tiles = hidden // HIDDEN_TILE, model // MODEL_TILE
    chips = devices // 2

    me = lax.axis_index("tp")
    chip, core = me // 2, lax.rem(me, 2)
    right = {"tp": lax.rem(chip + 1, chips) * 2 + core}
    left = {"tp": lax.rem(chip + chips - 1, chips) * 2 + core}
    sibling = {"tp": chip * 2 + 1 - core}

    theirs, ours = pl.ds(0, rows), pl.ds(rows, rows)
    lo, hi = pl.ds(rows, half), pl.ds(rows + half, half)

    def remote(src, dst, send, recv, to):
        return pltpu.make_async_remote_copy(
            src_ref=src, dst_ref=dst, send_sem=send, recv_sem=recv, device_id=to, device_id_type=pl.DeviceIdType.MESH
        )

    loads = [
        pltpu.make_async_copy(src, dst, load_sem.at[i])
        for i, (src, dst) in enumerate([(x_hbm, xb.at[0, ours]), (wg_hbm, wg), (wu_hbm, wu), (wd_hbm, wd)])
    ]

    barrier = pltpu.get_barrier_semaphore()

    def greet(peer):
        pl.semaphore_signal(barrier, inc=1, device_id=peer, device_id_type=pl.DeviceIdType.MESH)

    @pl.when(core == 0)
    def _():
        greet(right)
        pl.semaphore_wait(barrier, 2)

    @pl.when(core == 1)
    def _():
        greet(left)
        greet(sibling)
        pl.semaphore_wait(barrier, 1)

    top, bottom = pl.ds(0, half), pl.ds(half, half)
    early = [
        remote(x_hbm.at[top], xb.at[1, lo], ag_send.at[0], ag_recv.at[0], right),
        remote(x_hbm.at[bottom], xb.at[1, hi], ag_send.at[1], ag_recv.at[1], left),
    ]
    late = [
        remote(x_hbm.at[pl.ds(src + start, size)], xb.at[2, pl.ds(dst + start, size)], ag_send.at[i], ag_recv.at[i], to)
        for i, (src, dst, to, start, size) in enumerate(
            [
                (half, rows, right, 0, HEAD),
                (0, rows + half, left, 0, HEAD),
                (half, rows, right, HEAD, half - HEAD),
                (0, rows + half, left, HEAD, half - HEAD),
            ],
            2,
        )
    ]
    relays = [
        remote(xb.at[1, lo], xb.at[3, lo], ag_send.at[6], ag_recv.at[6], right),
        remote(xb.at[1, hi], xb.at[3, hi], ag_send.at[7], ag_recv.at[7], left),
    ]
    passes = [
        remote(xb.at[q, ours] if q else x_hbm, xb.at[q, theirs], pass_send.at[q], pass_recv.at[q], sibling) for q in range(4)
    ]

    def tell(sem, peer):
        pl.semaphore_signal(sem, inc=1, device_id=peer, device_id_type=pl.DeviceIdType.MESH)

    @pl.when(core == 0)
    def _():
        tell(seen, left)
        early[1].start()
        late[1].start()
        tell(mate, sibling)
        passes[0].start()
        pl.semaphore_wait(seen, 1)
        early[0].start()
        late[0].start()

    @pl.when(core == 1)
    def _():
        tell(seen, right)
        early[0].start()
        late[0].start()
        pl.semaphore_wait(seen, 1)
        early[1].start()
        late[1].start()
        pl.semaphore_wait(mate, 1)
        passes[0].start()

    for load in loads:
        load.start()

    def gate_up(q, keep):
        @pl.loop(0, hidden_tiles)
        def _(n):
            cols = tile(n, HIDDEN_TILE)
            gate = jnp.dot(xb[q], wg[:, cols], preferred_element_type=F32)
            up = jnp.dot(xb[q], wu[:, cols], preferred_element_type=F32)
            h = (jax.nn.silu(gate) * up).astype(BF16)
            work[:, cols] = h[:rows]
            kept[keep, :, cols] = h[rows:]

    def to_sibling(q, n):
        cols = tile(n, MODEL_TILE)
        return remote(xb.at[q, theirs, cols], sib.at[q, :, cols], sib_send.at[q, n], sib_recv.at[q, n], sibling)

    def down_theirs(q):
        @pl.loop(0, model_tiles)
        def _(n):
            cols = tile(n, MODEL_TILE)
            term = jnp.dot(work[...], wd[:, cols], preferred_element_type=F32)
            xb[q, theirs, cols] = term.astype(BF16)
            to_sibling(q, n).start()

    def from_sibling(q):
        @pl.loop(0, model_tiles)
        def _(n):
            to_sibling(q, n).wait_recv()

    def pair_sum(q, keep, cols):
        term = jnp.dot(kept[keep], wd[:, cols], preferred_element_type=F32)
        return term + sib[q, :, cols].astype(F32)

    def pure_hops():
        return (
            remote(xb.at[0, top], pure.at[top], pure_send.at[0], pure_recv.at[0], left),
            remote(xb.at[0, bottom], pure.at[bottom], pure_send.at[1], pure_recv.at[1], right),
        )

    pieces = [pl.ds(0, model - LAST), pl.ds(model - LAST, LAST)]

    def first_hops(n):
        cols = pieces[n]
        return (
            remote(xb.at[3, lo, cols], first.at[bottom, cols], first_send.at[0, n], first_recv.at[0, n], right),
            remote(xb.at[3, hi, cols], first.at[top, cols], first_send.at[1, n], first_recv.at[1, n], left),
        )

    def second_hops(n):
        cols = pieces[n]
        return (
            remote(xb.at[2, lo, cols], second.at[bottom, cols], second_send.at[0, n], second_recv.at[0, n], left),
            remote(xb.at[2, hi, cols], second.at[top, cols], second_send.at[1, n], second_recv.at[1, n], right),
        )

    for load in loads:
        load.wait()
    passes[0].wait_recv()
    gate_up(0, 0)
    down_theirs(0)

    for copy in early:
        copy.wait_recv()
    for copy in (*relays, *late[2:], passes[1]):
        copy.start()
    passes[1].wait_recv()
    gate_up(1, 2)
    down_theirs(1)
    from_sibling(1)

    @pl.loop(0, model_tiles)
    def _(n):
        cols = tile(n, MODEL_TILE)
        to_sibling(0, n).wait_send()
        xb[0, theirs, cols] = pair_sum(1, 2, cols).astype(BF16)

    for copy in pure_hops():
        copy.start()

    for copy in relays:
        copy.wait_recv()
    passes[3].start()
    passes[3].wait_recv()
    gate_up(3, 2)
    down_theirs(3)
    passes[3].wait_send()
    from_sibling(3)

    @pl.loop(0, model_tiles)
    def _(n):
        cols = tile(n, MODEL_TILE)
        xb[3, ours, cols] = pair_sum(3, 2, cols).astype(BF16)

    for n in range(2):
        for copy in first_hops(n):
            copy.start()

    for copy in late:
        copy.wait_recv()
    passes[2].start()
    passes[2].wait_recv()
    gate_up(2, 1)
    down_theirs(2)
    passes[2].wait_send()
    from_sibling(2)

    @pl.loop(0, model_tiles)
    def _(n):
        cols = tile(n, MODEL_TILE)
        total[:, cols] = pair_sum(2, 1, cols)

    for n in range(2):
        for copy, onward, half_rows, dst in zip(first_hops(n), second_hops(n)[::-1], (bottom, top), (hi, lo)):
            copy.wait_recv()
            held = total[half_rows, pieces[n]] + first[half_rows, pieces[n]].astype(F32)
            xb[2, dst, pieces[n]] = held.astype(BF16)
            onward.start()

    from_sibling(0)
    for copy in pure_hops():
        copy.wait_recv()

    @pl.loop(0, model_tiles)
    def _(n):
        cols = tile(n, MODEL_TILE)
        total[:, cols] = pair_sum(0, 0, cols) + pure[:, cols].astype(F32)
        for q in range(1, 4):
            to_sibling(q, n).wait_send()

    for copy in (*early, *late, *relays, *passes[:2], *pure_hops(), *first_hops(0), *first_hops(1)):
        copy.wait_send()
    for n in range(2):
        for copy, half_rows in zip(second_hops(n), (bottom, top)):
            copy.wait_recv()
            held = total[half_rows, pieces[n]] + second[half_rows, pieces[n]].astype(F32)
            y[half_rows, pieces[n]] = held.astype(BF16)

    for copy in (*second_hops(0), *second_hops(1)):
        copy.wait_send()


def solution(mesh):
    devices = mesh.shape["tp"]

    def step(x, w_gate, w_up, w_down):
        rows, model = x.shape
        hidden = w_gate.shape[1]
        tiles = model // MODEL_TILE
        dma = pltpu.SemaphoreType.DMA
        return pl.pallas_call(
            functools.partial(kernel, devices),
            out_shape=pltpu.VMEM((rows, model), BF16),
            in_specs=[pl.BlockSpec(memory_space=pl.ANY)] * 4,
            out_specs=pl.BlockSpec(memory_space=pltpu.VMEM),
            scratch_shapes=[
                pltpu.VMEM((model, hidden), BF16),
                pltpu.VMEM((model, hidden), BF16),
                pltpu.VMEM((hidden, model), BF16),
                pltpu.VMEM((4, 2 * rows, model), BF16),
                pltpu.VMEM((4, rows, model), BF16),
                pltpu.VMEM((rows, model), BF16),
                pltpu.VMEM((rows, model), BF16),
                pltpu.VMEM((rows, model), BF16),
                pltpu.VMEM((rows, model), F32),
                pltpu.VMEM((rows, hidden), BF16),
                pltpu.VMEM((3, rows, hidden), BF16),
                dma((4,)),
                dma((8,)), dma((8,)), dma((4,)), dma((4,)),
                dma((4, tiles)), dma((4, tiles)),
                dma((2, 2)), dma((2, 2)),
                dma((2,)), dma((2,)),
                dma((2, 2)), dma((2, 2)),
                pltpu.SemaphoreType.REGULAR, pltpu.SemaphoreType.REGULAR,
            ],
            compiler_params=pltpu.CompilerParams(
                collective_id=0, has_side_effects=True, vmem_limit_bytes=64_000_000
            ),
        )(x, w_gate, w_up, w_down)

    return jax.shard_map(
        step,
        mesh=mesh,
        in_specs=(P(("dp", "tp"), None), P(None, "tp"), P(None, "tp"), P("tp", None)),
        out_specs=P(("dp", "tp"), None),
        check_vma=False,
    )
```
